256 devices in a mesh: rep: 4 (over x), fsdp: 64 (over y, z, core).
Axes of the slice: x: 4, y: 4, z: 8, core: 2. Of those that a mesh axis runs over, the one named last changes fastest.
Arguments:
- params: bfloat16 [2, 8192, 4608], P(None, 'fsdp'), may hold values from -6 to 6
- deltas: bfloat16 [4, 2, 8192, 4608], P('rep', None, 'fsdp'), may hold values from -3 to 3
- momentum: float32 [2, 8192, 4608], P(None, 'fsdp', 'rep'), may hold values from -2 to 2
Outputs:
- new_params: bfloat16 [2, 8192, 4608], P(None, 'fsdp')
- new_momentum: float32 [2, 8192, 4608], P(None, 'fsdp', 'rep')
The draws below stay inside these ranges and needn't reach their ends.
All inputs are finite; a program needn't handle non-finite values.
Results may differ from the reference program's by a relative error of at most 0.0035.
Values may be sent and summed in bfloat16 or wider, within the bound.
No kernel may reach another device: no remote copies, remote signals or barrier semaphores. Data moves between devices by JAX's collectives and lax.ppermute only.
A program may use at most 64 MiB of HBM per device.

```python
import math
import jax
import jax.numpy as jnp

D = 4608
Q_ROWS = 4096
KV_ROWS = 2048
LAYERS = 2
ROWS = 8192
REPLICAS = 4


def draw_deltas(key, part):
    subkeys = jax.random.split(key, 10)
    row_index = jnp.arange(ROWS, dtype=jnp.int32)
    tensor = (row_index >= Q_ROWS).astype(jnp.int32) + (row_index >= Q_ROWS + KV_ROWS).astype(jnp.int32)
    first_row = jnp.where(tensor == 0, 0, jnp.where(tensor == 1, Q_ROWS, Q_ROWS + KV_ROWS))
    extent = jnp.where(tensor == 0, Q_ROWS, KV_ROWS)
    position = (row_index - first_row).astype(jnp.float32) / extent.astype(jnp.float32)
    amplitude = jnp.exp(jax.random.uniform(subkeys[0], (LAYERS, 3), jnp.float32, math.log(0.1), 0.0))
    replica_amp = jnp.exp(jax.random.uniform(subkeys[1], (REPLICAS, LAYERS, 3), jnp.float32, math.log(0.5), 0.0))
    cycles = jax.random.randint(subkeys[2], (LAYERS, 3), 1, 3).astype(jnp.float32)
    offset = jax.random.uniform(subkeys[9], (LAYERS, 3), jnp.float32, 0.0, 2.0 * math.pi)
    ripple = 0.5 * (1.0 + jnp.sin(2.0 * math.pi * cycles[:, tensor] * position[None, :] + offset[:, tensor]))
    profile = jnp.exp(math.log(0.1) * ripple)
    jitter = jnp.exp(jax.random.uniform(subkeys[4], (LAYERS, ROWS), jnp.float32, math.log(0.5), 0.0))
    columns = jnp.exp(jax.random.uniform(subkeys[5], (LAYERS, D), jnp.float32, math.log(0.1), 0.0))
    signal = jax.random.uniform(subkeys[8], (REPLICAS, LAYERS, ROWS, D), jnp.float32, -1.0, 1.0)
    row_scale = amplitude[:, tensor] * profile * jitter
    values = 3.0 * replica_amp[:, :, tensor][..., None] * row_scale[None, :, :, None] * columns[None, :, None, :] * signal
    return values.astype(jnp.bfloat16)


def levels(stream_key, shape, cuts, low, top_value):
    loudness, own = 1.0, jax.random.fold_in(stream_key, 6)
    for dim, blocks in cuts:
        heights = jnp.exp(jax.random.uniform(jax.random.fold_in(own, dim), (blocks,), jnp.float32, low / len(cuts), top_value / len(cuts)))
        loudness = loudness * jnp.repeat(heights, shape[dim] // blocks).reshape([-1 if axis == dim else 1 for axis in range(len(shape))])
    return loudness


def noise(key, dims, width, most, cuts=(), kind=jnp.bfloat16):
    values = width * jax.random.normal(key, dims, jnp.float32)
    if cuts:
        values = values * levels(key, dims, cuts, -0.22, 0.18)
    return jnp.clip(values, -most, most).astype(kind)


def setup_inputs(seed: int = 0) -> dict:
    seeds = jax.random.split(jax.random.key(seed), 4)
    return {
        "params": noise(seeds[0], (LAYERS, ROWS, D), 1.0, 6.0, ((1, 64),)),
        "deltas": draw_deltas(jax.random.fold_in(seeds[3], 71), 0),
        "momentum": noise(seeds[2], (LAYERS, ROWS, D), 0.3, 2.0, ((1, 64), (2, 4)), jnp.float32),
    }


clip_share = 0.5
peak_eps = 1e-6
outer_rate = 0.7
momentum_decay = 0.9


def reference(params, deltas, momentum):
    row_ids = jnp.arange(ROWS, dtype=jnp.int32)
    tensor_ids = (row_ids >= Q_ROWS).astype(jnp.int32) + (row_ids >= Q_ROWS + KV_ROWS).astype(jnp.int32)
    row_peak = jnp.max(jnp.max(jnp.abs(deltas), axis=3), axis=0).astype(jnp.float32)
    member = tensor_ids[None, :] == jnp.arange(3, dtype=jnp.int32)[:, None]
    peak = jnp.max(jnp.where(member[None], row_peak[:, None, :], jnp.float32(0.0)), axis=2)
    scaled = clip_share * (peak + peak_eps)
    tau = jnp.sum(jnp.where(member[None], scaled[:, :, None], jnp.float32(0.0)), axis=1)
    total = jnp.zeros((LAYERS, ROWS, D), jnp.float32)
    for replica in range(REPLICAS):
        codes = jnp.clip(deltas[replica].astype(jnp.float32) / tau[..., None], -1.0, 1.0).astype(jnp.bfloat16)
        total = total + codes.astype(jnp.float32)
    outer = tau[..., None] * total / jnp.float32(REPLICAS)
    new_momentum = momentum_decay * momentum + outer
    new_params = (params.astype(jnp.float32) - outer_rate * (outer + momentum_decay * new_momentum)).astype(jnp.bfloat16)
    return new_params, new_momentum
```

```python
import functools

import jax
import jax.numpy as jnp
from jax import lax
from jax.experimental import pallas as pl
from jax.experimental.pallas import tpu as pltpu
from jax.sharding import Mesh
from jax.sharding import PartitionSpec as P


Q_ROWS = 4096
KV_ROWS = 2048
FSDP = ("fsdp_0", "fsdp_1", "fsdp_2")
REP = 4

clip_share = 0.5
peak_eps = 1e-06
outer_rate = 0.7
momentum_decay = 0.9


def part_kernel(me_ref, local_ref, b2_ref, b1_ref, b3_ref, top_ref):
    owned = b1_ref.shape[2]
    me = me_ref[0]
    step = local_ref.shape[1]
    first = pl.multiple_of(pl.program_id(0) * step, step)
    for ahead, ref in ((2, b2_ref), (1, b1_ref), (3, b3_ref)):
        start = pl.multiple_of(lax.rem(me + ahead, REP) * owned, 128)
        ref[:, pl.ds(first, step), :] = local_ref[:, :, pl.ds(start, owned)]
    size = jnp.max(jnp.abs(local_ref[...]).astype(jnp.float32), axis=2, keepdims=True)
    size = jnp.max(size, axis=1)

    @pl.when(pl.program_id(0) == 0)
    def _():
        top_ref[...] = jnp.zeros_like(top_ref)

    top_ref[...] = jnp.maximum(top_ref[...], jnp.broadcast_to(size, top_ref.shape))


def parts_and_top(local, me, owned):
    layers, rows, width = local.shape
    step = 32
    block = pl.BlockSpec(memory_space=pltpu.VMEM)
    piece = jax.ShapeDtypeStruct((layers, rows, owned), local.dtype)
    return pl.pallas_call(
        part_kernel,
        grid_spec=pltpu.PrefetchScalarGridSpec(
            num_scalar_prefetch=1,
            grid=(rows // step,),
            in_specs=[pl.BlockSpec((layers, step, width), lambda i, me: (0, i, 0))],
            out_specs=[block, block, block, pl.BlockSpec((layers, 128), lambda i, me: (0, 0))],
        ),
        out_shape=[piece, piece, piece, jax.ShapeDtypeStruct((layers, 128), jnp.float32)],
        name="parts_and_top",
    )(me, local)


def update_kernel(layer, me_ref, tau_ref, own_ref, r2_ref, r1_ref, r3_ref, p_ref, m_ref, *rest):
    fresh_ref, new_ref = rest[-2:]
    tau = tau_ref[layer]
    inverse = tau_ref[layer + 2]
    total = None
    step = own_ref.shape[1]
    here = pl.ds(pl.multiple_of(pl.program_id(0) * step, step), step)
    blocks = (own_ref[0], r1_ref[layer, here], r2_ref[layer, here], r3_ref[layer, here])
    for block in blocks:
        code = jnp.clip(block.astype(jnp.float32) * inverse, -1.0, 1.0)
        code = code.astype(jnp.bfloat16).astype(jnp.float32)
        total = code if total is None else total + code
    outer = (tau / REP) * total
    fresh_moment = momentum_decay * m_ref[0] + outer
    fresh = p_ref[0].astype(jnp.float32) - outer_rate * (outer + momentum_decay * fresh_moment)
    fresh_ref[here] = fresh.astype(jnp.bfloat16)
    new_ref[0] = fresh_moment


def update(layer, me, tau, local, received, params, momentum, earlier):
    _, rows, owned = momentum.shape
    step = 32
    mine = pl.BlockSpec((1, step, owned), lambda i, me, tau: (layer, i, me[0]))
    flat = pl.BlockSpec((1, step, owned), lambda i, me, tau: (layer, i, 0))
    operands = [local, *received, params, momentum]
    whole = pl.BlockSpec(memory_space=pltpu.VMEM)
    specs = [mine, whole, whole, whole, mine, flat]
    aliases = {}
    if earlier is not None:
        operands.append(earlier)
        specs.append(pl.BlockSpec(memory_space=pl.ANY))
        aliases = {len(operands) + 1: 1}
    return pl.pallas_call(
        functools.partial(update_kernel, layer),
        grid_spec=pltpu.PrefetchScalarGridSpec(
            num_scalar_prefetch=2,
            grid=(rows // step,),
            in_specs=specs,
            out_specs=[whole, flat],
        ),
        out_shape=[
            jax.ShapeDtypeStruct((rows, owned), jnp.bfloat16),
            jax.ShapeDtypeStruct(momentum.shape, jnp.float32),
        ],
        input_output_aliases=aliases,
    )(me, tau, *operands)


def place_kernel(moves, me_ref, *refs):
    sems = refs[-1]
    out_ref = refs[-2]
    copies = []
    for k, (layer, back, first, count) in enumerate(moves):
        src = refs[k]
        owned = src.shape[-1]
        start = pl.multiple_of(lax.rem(me_ref[0] + back, REP) * owned, 128)
        dst = out_ref.at[layer, pl.ds(first, count), pl.ds(start, owned)]
        copies.append(pltpu.make_async_copy(src, dst, sems.at[k]))
    for copy in copies:
        copy.start()
    for copy in copies:
        copy.wait()


def place(me, moves, pieces, shape, earlier):
    operands = list(pieces)
    aliases = {}
    if earlier is not None:
        operands.append(earlier)
        aliases = {len(operands): 0}
    return pl.pallas_call(
        functools.partial(place_kernel, moves),
        in_specs=[pl.BlockSpec(memory_space=pltpu.SMEM)]
        + [pl.BlockSpec(memory_space=pltpu.VMEM)] * len(pieces)
        + [pl.BlockSpec(memory_space=pl.ANY)] * len(aliases),
        out_specs=pl.BlockSpec(memory_space=pl.ANY),
        out_shape=jax.ShapeDtypeStruct(shape, jnp.bfloat16),
        scratch_shapes=[pltpu.SemaphoreType.DMA((len(moves),))],
        input_output_aliases=aliases,
        name="place",
    )(me, *operands)


def spread(value, axes):
    copies = jnp.broadcast_to(value, (lax.axis_size(axes), *value.shape))
    return lax.all_to_all(copies, axes, 0, 0, tiled=True)


def tensor_of(y, rows):
    first = y * (16 * rows)
    return (first >= Q_ROWS).astype(jnp.int32) + (first >= Q_ROWS + KV_ROWS).astype(jnp.int32)


def shift(value, by):
    return lax.ppermute(value, "rep", [(i, (i + by) % REP) for i in range(REP)])


def on_device(params, deltas, momentum):
    local = deltas[0]
    _, rows, owned = momentum.shape
    me = lax.axis_index("rep").reshape(1)
    b2, b1, b3, top = parts_and_top(local, me, owned)
    r2 = shift(b2, 2)
    r1 = shift(b1, 1)
    r3 = shift(b3, 3)
    top = jnp.max(spread(top[:, 0], ("fsdp_1", "fsdp_2")), axis=0)
    tops = spread(top, ("rep", "fsdp_0"))
    ys = lax.rem(lax.iota(jnp.int32, 16), 4)
    same = (tensor_of(ys, rows) == tensor_of(lax.axis_index("fsdp_0"), rows))[:, None]
    tau = clip_share * (jnp.max(jnp.where(same, tops, 0.0), axis=0) + peak_eps)
    tau = jnp.concatenate([tau, 1.0 / tau])
    received = (r2, r1, r3)
    fresh0, new_m = update(0, me, tau, local, received, params, momentum, None)
    right0, left0 = shift(fresh0, 1), shift(fresh0, 3)
    fresh1, new_m = update(1, me, tau, local, received, params, momentum, new_m)
    right1, left1 = shift(fresh1, 1), shift(fresh1, 3)
    half = rows // 2
    far0 = (shift(right0[:half], 1), shift(left0[half:], 3))
    far1 = (shift(right1[:half], 1), shift(left1[half:], 3))
    moves = [(l, b, 0, rows) for l in range(2) for b in (0, 3, 1)]
    out = place(me, moves, (fresh0, right0, left0, fresh1, right1, left1), params.shape, None)
    moves = [(l, 2, f, half) for l in range(2) for f in (0, half)]
    out = place(me, moves, (*far0, *far1), params.shape, out)
    return out, new_m


def solution(mesh):
    torus = Mesh(
        mesh.devices.reshape(mesh.shape["rep"], 4, 8, 2), ("rep", "fsdp_0", "fsdp_1", "fsdp_2")
    )
    placed = (P(None, FSDP, None), P("rep", None, FSDP, None), P(None, FSDP, "rep"))
    return jax.shard_map(
        on_device,
        mesh=torus,
        in_specs=placed,
        out_specs=(P(None, FSDP, None), P(None, FSDP, "rep")),
        check_vma=False,
    )
```

```python
import functools

import jax
import jax.numpy as jnp
from jax import lax
from jax.experimental import pallas as pl
from jax.experimental.pallas import tpu as pltpu
from jax.sharding import Mesh
from jax.sharding import PartitionSpec as P


Q_ROWS = 4096
KV_ROWS = 2048
FSDP = ("y_hi", "y_lo", "z", "core")
AXES = ("rep", *FSDP)
SIZES = (4, 2, 2, 8, 2)
REP = 4

clip_share = 0.5
peak_eps = 1e-06
outer_rate = 0.7
momentum_decay = 0.9

VMEM = pltpu.VMEM
SMALL = pltpu.CompilerParams(vmem_limit_bytes=4 * 1024 * 1024)
WHOLE = pl.BlockSpec(memory_space=pltpu.VMEM)
HBM = pl.BlockSpec(memory_space=pl.ANY)


def far(array):
    return pltpu.with_memory_space_constraint(array, pltpu.HBM)


def near(*arrays):
    return tuple(pltpu.with_memory_space_constraint(a, pltpu.VMEM) for a in arrays)


def columns(me, back, owned):
    return pl.ds(pl.multiple_of(lax.rem(me + back, REP) * owned, 128), owned)


def cut_kernel(aheads, me_ref, local_ref, *refs):
    outs, sems = refs[:-1], refs[-1]
    owned = outs[0].shape[-1]
    copies = []
    for k, (out, (layer, count, ahead)) in enumerate(zip(outs, aheads, strict=True)):
        src = local_ref.at[pl.ds(layer, count), :, columns(me_ref[0], ahead, owned)]
        copies.append(pltpu.make_async_copy(src, out, sems.at[k]))
    for copy in copies:
        copy.start()
    for copy in copies:
        copy.wait()


def cut(local, me, owned, aheads):
    pieces = [VMEM((n, local.shape[1], owned), local.dtype) for _, n, _ in aheads]
    return pl.pallas_call(
        functools.partial(cut_kernel, aheads),
        in_specs=[pl.BlockSpec(memory_space=pltpu.SMEM), HBM],
        out_specs=[WHOLE] * len(aheads),
        out_shape=pieces,
        scratch_shapes=[pltpu.SemaphoreType.DMA((len(aheads),))],
        compiler_params=SMALL,
        name="cut",
    )(me, far(local))


def stage_kernel(me_ref, local_ref, params_ref, moment_ref, own_ref, piece_ref, held_ref, sems):
    mine = columns(me_ref[0], 0, piece_ref.shape[-1])
    copies = (
        pltpu.make_async_copy(local_ref.at[:, :, mine], own_ref, sems.at[0]),
        pltpu.make_async_copy(params_ref.at[:, :, mine], piece_ref, sems.at[1]),
        pltpu.make_async_copy(moment_ref, held_ref, sems.at[2]),
    )
    for copy in copies:
        copy.start()
    for copy in copies:
        copy.wait()


def stage(me, local, params, momentum):
    shape = momentum.shape
    return pl.pallas_call(
        stage_kernel,
        in_specs=[pl.BlockSpec(memory_space=pltpu.SMEM), HBM, HBM, HBM],
        out_specs=[WHOLE, WHOLE, WHOLE],
        out_shape=[VMEM(shape, local.dtype), VMEM(shape, params.dtype), VMEM(shape, jnp.float32)],
        scratch_shapes=[pltpu.SemaphoreType.DMA((3,))],
        compiler_params=SMALL,
        name="stage",
    )(me, far(local), far(params), far(momentum))


def top_kernel(local_ref, out_ref):
    tops = []
    for layer in range(local_ref.shape[0]):
        size = jnp.max(jnp.abs(local_ref[layer]).reshape(8, 16, -1), axis=0)
        tops.append(jnp.max(size.astype(jnp.float32), axis=(0, 1), keepdims=True))
    lane = lax.broadcasted_iota(jnp.int32, out_ref.shape, 1)
    out_ref[...] = jnp.where(lane < out_ref.shape[1] // 2, tops[0], tops[1])


def top_of(local):
    return pl.pallas_call(
        top_kernel,
        in_specs=[WHOLE],
        out_specs=WHOLE,
        out_shape=VMEM((1, 128), jnp.float32),
        compiler_params=SMALL,
        name="top",
    )(*near(local))


def update_kernel(layer, *refs):
    like_ref, top_ref, own_ref, r2_ref, r1_ref, r3_ref, piece_ref, moment_ref, fresh_ref, new_ref = refs
    mates = top_ref.shape[0] // like_ref.shape[0]
    seen = None
    for y in range(like_ref.shape[0]):
        top = jnp.max(top_ref[pl.ds(y * mates, mates)], axis=0)
        top = jnp.where(like_ref[y] == 1, top, 0.0)
        seen = top if seen is None else jnp.maximum(seen, top)
    lane = lax.broadcasted_iota(jnp.int32, seen.shape, 1)
    seen = jnp.where(lane // (seen.shape[1] // 2) == layer, seen, 0.0)
    peak = jnp.max(seen, axis=(0, 1), keepdims=True)
    tau = clip_share * (peak + peak_eps)
    inverse = 1.0 / tau
    quarter = tau * (1.0 / REP)
    _, owned = fresh_ref.shape
    for start in range(0, owned, 128):
        cols = pl.ds(start, 128)
        total = None
        for ref in (own_ref, r1_ref, r2_ref, r3_ref):
            at = min(layer, ref.shape[0] - 1)
            code = jnp.clip(ref[at, :, cols].astype(jnp.float32) * inverse, -1.0, 1.0)
            code = code.astype(jnp.bfloat16).astype(jnp.float32)
            total = code if total is None else total + code
        outer = quarter * total
        fresh_moment = momentum_decay * moment_ref[layer, :, cols] + outer
        fresh = piece_ref[layer, :, cols].astype(jnp.float32)
        fresh = fresh - outer_rate * (outer + momentum_decay * fresh_moment)
        fresh_ref[:, cols] = fresh.astype(jnp.bfloat16)
        new_ref[:, cols] = fresh_moment


def update(layer, like, tops, blocks, piece, moment):
    rows, owned = moment.shape[1:]
    operands = near(tops, *blocks, piece, moment)
    return pl.pallas_call(
        functools.partial(update_kernel, layer),
        in_specs=[pl.BlockSpec(memory_space=pltpu.SMEM)] + [WHOLE] * len(operands),
        out_specs=[WHOLE, WHOLE],
        out_shape=[VMEM((rows, owned), jnp.bfloat16), VMEM((rows, owned), jnp.float32)],
        compiler_params=SMALL,
    )(like, *operands)


def place_kernel(moves, count, me_ref, *refs):
    sems, outs = refs[-1], refs[-1 - count : -1]
    copies = []
    for k, (which, layer, back, first, height) in enumerate(moves):
        src = refs[k]
        owned = src.shape[-1]
        here = columns(me_ref[0], back, owned) if which == 0 else pl.ds(0, owned)
        dst = outs[which].at[layer, pl.ds(first, height), here]
        copies.append(pltpu.make_async_copy(src, dst, sems.at[k]))
    for copy in copies:
        copy.start()
    for copy in copies:
        copy.wait()


def place(me, moves, pieces, shapes, earlier):
    operands = list(near(*pieces))
    aliases = {}
    if earlier is not None:
        aliases = {1 + len(operands) + k: k for k in range(len(earlier))}
        operands += earlier
    return pl.pallas_call(
        functools.partial(place_kernel, moves, len(shapes)),
        in_specs=[pl.BlockSpec(memory_space=pltpu.SMEM)]
        + [WHOLE] * len(pieces)
        + [HBM] * len(aliases),
        out_specs=[HBM] * len(shapes),
        out_shape=shapes,
        scratch_shapes=[pltpu.SemaphoreType.DMA((len(moves),))],
        input_output_aliases=aliases,
        compiler_params=SMALL,
        name="place",
    )(me, *operands)


def shift(value, by):
    return lax.ppermute(value, "rep", [(i, (i + by) % REP) for i in range(REP)])


def tensor_of(y, rows):
    first = y * SIZES[3] * SIZES[4] * rows
    return (first >= Q_ROWS).astype(jnp.int32) + (first >= Q_ROWS + KV_ROWS).astype(jnp.int32)


def on_device(params, deltas, momentum):
    local = deltas[0]
    _, rows, owned = momentum.shape
    me = lax.axis_index("rep").reshape(1)
    b01, b03, b2 = cut(local, me, owned, ((0, 1, 1), (0, 1, 3), (0, 2, 2)))
    top = top_of(local)
    tops = [top, *(shift(top, d) for d in (1, 3, 2))]
    r01, r03 = shift(b01, 1), shift(b03, 3)
    r2 = shift(b2, 2)
    b11, b13 = cut(local, me, owned, ((1, 1, 1), (1, 1, 3)))
    r11, r13 = shift(b11, 1), shift(b13, 3)
    received = [(r2, r01, r03), (r2, r11, r13)]
    y_hi = lax.axis_index("y_hi") * 2
    like = tensor_of(y_hi + lax.iota(jnp.int32, 2), rows) == tensor_of(y_hi + lax.axis_index("y_lo"), rows)
    like = like.astype(jnp.int32)
    top = functools.reduce(jnp.maximum, tops)
    top = jnp.broadcast_to(top[None], (32, 1, 128))
    tops = lax.all_to_all(top, ("y_lo", "z", "core"), 0, 0, tiled=True)
    own, piece, moment = stage(me, local, params, momentum)
    fresh0, new0 = update(0, like, tops, (own, *received[0]), piece, moment)
    right0, left0 = shift(fresh0, 1), shift(fresh0, 3)
    fresh1, new1 = update(1, like, tops, (own, *received[1]), piece, moment)
    right1, left1 = shift(fresh1, 1), shift(fresh1, 3)
    half = rows // 2
    farr0, farl0 = shift(right0[:half], 1), shift(left0[half:], 3)
    farr1, farl1 = shift(right1[:half], 1), shift(left1[half:], 3)
    shapes = [
        jax.ShapeDtypeStruct(params.shape, params.dtype),
        jax.ShapeDtypeStruct(momentum.shape, momentum.dtype),
    ]
    moves = [(0, l, b, 0, rows) for l in range(2) for b in (0, 3, 1)]
    moves += [(1, 0, 0, 0, rows), (1, 1, 0, 0, rows)]
    pieces = (fresh0, right0, left0, fresh1, right1, left1, new0, new1)
    out, new_m = place(me, moves, pieces, shapes, None)
    moves = [(0, l, 2, f, half) for l in range(2) for f in (0, half)]
    (out,) = place(me, moves, (farr0, farl0, farr1, farl1), shapes[:1], (out,))
    return out, new_m


def solution(mesh):
    torus = Mesh(mesh.devices.reshape(SIZES), AXES)
    placed = (P(None, FSDP, None), P("rep", None, FSDP, None), P(None, FSDP, "rep"))
    return jax.shard_map(
        on_device,
        mesh=torus,
        in_specs=placed,
        out_specs=(P(None, FSDP, None), P(None, FSDP, "rep")),
        check_vma=False,
    )
```

```python
import functools

import jax
import jax.numpy as jnp
from jax import lax
from jax.experimental import pallas as pl
from jax.experimental.pallas import tpu as pltpu
from jax.sharding import Mesh
from jax.sharding import PartitionSpec as P


Q_ROWS = 4096
KV_ROWS = 2048
FSDP = ("y_hi", "y_lo", "z", "core")
AXES = ("rep", *FSDP)
SIZES = (4, 2, 2, 8, 2)
REP = 4

clip_share = 0.5
peak_eps = 1e-06
outer_rate = 0.7
momentum_decay = 0.9

VMEM = pltpu.VMEM
SMALL = pltpu.CompilerParams(vmem_limit_bytes=4 * 1024 * 1024)
WHOLE = pl.BlockSpec(memory_space=pltpu.VMEM)
SCALARS = pl.BlockSpec(memory_space=pltpu.SMEM)
HBM = pl.BlockSpec(memory_space=pl.ANY)


def far(array):
    return pltpu.with_memory_space_constraint(array, pltpu.HBM)


def near(*arrays):
    return tuple(pltpu.with_memory_space_constraint(a, pltpu.VMEM) for a in arrays)


def columns(ahead, owned):
    return pl.ds(pl.multiple_of(lax.rem(lax.axis_index("rep") + ahead, REP) * owned, 128), owned)


def run_all(copies):
    for copy in copies:
        copy.start()
    for copy in copies:
        copy.wait()


def open_kernel(moves, local_ref, *refs):
    outs, (top_ref, held_ref, sems) = refs[:-3], refs[-3:]
    layers, rows, width = local_ref.shape
    owned = width // REP
    count = sems.shape[0] // layers
    step = rows // count
    loads = []
    for layer in range(layers):
        for k in range(count):
            here = (layer, pl.ds(k * step, step))
            sem = sems.at[layer * count + k]
            loads.append(pltpu.make_async_copy(local_ref.at[here], held_ref.at[here], sem))
    for load in loads:
        load.start()
    tops = []
    for layer in range(layers):
        size = None
        for k in range(count):
            loads[layer * count + k].wait()
            here = slice(k * step, (k + 1) * step)
            for which, at, first, last, ahead in moves[layer]:
                if first <= k * step < last:
                    block = held_ref[layer, here, columns(ahead, owned)]
                    outs[which][(*at, here)] = block
            chunk = jnp.max(jnp.abs(held_ref[layer, here]).reshape(step // 16, 16, width), axis=0)
            size = chunk if size is None else jnp.maximum(size, chunk)
        tops.append(jnp.max(size.astype(jnp.float32), axis=(0, 1), keepdims=True))
    lane = lax.broadcasted_iota(jnp.int32, top_ref.shape, 1)
    top_ref[...] = jnp.where(lane < top_ref.shape[1] // 2, tops[0], tops[1])


def open_up(local, moves, shapes):
    outs = [VMEM(shape, local.dtype) for shape in shapes]
    outs += [VMEM((1, 128), jnp.float32)]
    return pl.pallas_call(
        functools.partial(open_kernel, moves),
        in_specs=[HBM],
        out_specs=[WHOLE] * len(outs),
        out_shape=outs,
        scratch_shapes=[VMEM(local.shape, local.dtype), pltpu.SemaphoreType.DMA((8,))],
        compiler_params=pltpu.CompilerParams(vmem_limit_bytes=8 * 1024 * 1024),
        name="open",
    )(far(local))


def load_kernel(moves, *refs):
    count = len(moves)
    sources, outs, sems = refs[: -count - 1], refs[-count - 1 : -1], refs[-1]
    owned = outs[0].shape[-1]
    copies = []
    for k, (which, at, ahead) in enumerate(moves):
        src = sources[which].at[at]
        if ahead is not None:
            src = sources[which].at[at, :, columns(ahead, owned)]
        copies.append(pltpu.make_async_copy(src, outs[k], sems.at[k]))
    run_all(copies)


def load(sources, moves, shapes):
    return pl.pallas_call(
        functools.partial(load_kernel, moves),
        in_specs=[HBM] * len(sources),
        out_specs=[WHOLE] * len(moves),
        out_shape=[VMEM(s, sources[m[0]].dtype) for s, m in zip(shapes, moves, strict=True)],
        scratch_shapes=[pltpu.SemaphoreType.DMA((len(moves),))],
        compiler_params=SMALL,
        name="load",
    )(*map(far, sources))


def meet_kernel(*refs):
    top = functools.reduce(jnp.maximum, [ref[...] for ref in refs[:-1]])
    refs[-1][...] = jnp.broadcast_to(top[None], refs[-1].shape)


def meet(tops, count):
    return pl.pallas_call(
        meet_kernel,
        in_specs=[WHOLE] * len(tops),
        out_specs=WHOLE,
        out_shape=VMEM((count, 1, 128), jnp.float32),
        compiler_params=SMALL,
        name="meet",
    )(*near(*tops))


def tau_of(like_ref, top_ref, layer):
    mates = top_ref.shape[0] // like_ref.shape[0]
    seen = None
    for y in range(like_ref.shape[0]):
        top = jnp.max(top_ref[pl.ds(y * mates, mates)], axis=0)
        top = jnp.where(like_ref[y] == 1, top, 0.0)
        seen = top if seen is None else jnp.maximum(seen, top)
    lane = lax.broadcasted_iota(jnp.int32, seen.shape, 1)
    seen = jnp.where(lane // (seen.shape[1] // 2) == layer, seen, 0.0)
    return clip_share * (jnp.max(seen, axis=(0, 1), keepdims=True) + peak_eps)


def code_of(block, inverse):
    code = jnp.clip(block.astype(jnp.float32) * inverse, -1.0, 1.0)
    return code.astype(jnp.bfloat16).astype(jnp.float32)


def update_kernel(layer, like_ref, top_ref, *refs):
    blocks, (piece_ref, moment_ref, fresh_ref, new_ref) = refs[:-4], refs[-4:]
    tau = tau_of(like_ref, top_ref, layer)
    inverse = 1.0 / tau
    quarter = tau * (1.0 / REP)
    _, owned = fresh_ref.shape
    for start in range(0, owned, 128):
        cols = pl.ds(start, 128)
        raw = [ref[layer, :, cols] if len(ref.shape) == 3 else ref[:, cols] for ref in blocks]
        total = functools.reduce(jnp.add, [code_of(block, inverse) for block in raw])
        outer = quarter * total
        fresh_moment = momentum_decay * moment_ref[:, cols] + outer
        fresh = piece_ref[:, cols].astype(jnp.float32)
        fresh = fresh - outer_rate * (outer + momentum_decay * fresh_moment)
        fresh_ref[:, cols] = fresh.astype(jnp.bfloat16)
        new_ref[:, cols] = fresh_moment


def update(layer, like, tops, blocks, piece, moment):
    rows, owned = moment.shape
    operands = near(tops, *blocks, piece, moment)
    return pl.pallas_call(
        functools.partial(update_kernel, layer),
        in_specs=[SCALARS] + [WHOLE] * len(operands),
        out_specs=[WHOLE, WHOLE],
        out_shape=[VMEM((rows, owned), jnp.bfloat16), VMEM((rows, owned), jnp.float32)],
        compiler_params=SMALL,
    )(like, *operands)


def place_kernel(moves, count, *refs):
    sems, outs = refs[-1], refs[-1 - count : -1]
    copies = []
    for k, (which, layer, back, first, height) in enumerate(moves):
        src = refs[k]
        owned = src.shape[-1]
        here = columns(back, owned) if which == 0 else pl.ds(0, owned)
        dst = outs[which].at[layer, pl.ds(first, height), here]
        copies.append(pltpu.make_async_copy(src, dst, sems.at[k]))
    run_all(copies)


def place(moves, pieces, shapes, earlier):
    operands = list(near(*pieces))
    aliases = {}
    if earlier is not None:
        aliases = {len(operands) + k: k for k in range(len(earlier))}
        operands += earlier
    return pl.pallas_call(
        functools.partial(place_kernel, moves, len(shapes)),
        in_specs=[WHOLE] * len(pieces) + [HBM] * len(aliases),
        out_specs=[HBM] * len(shapes),
        out_shape=shapes,
        scratch_shapes=[pltpu.SemaphoreType.DMA((len(moves),))],
        input_output_aliases=aliases,
        compiler_params=SMALL,
        name="place",
    )(*operands)


def shift(value, by):
    return lax.ppermute(value, "rep", [(i, (i + by) % REP) for i in range(REP)])


def tensor_of(y, rows):
    first = y * SIZES[3] * SIZES[4] * rows
    return (first >= Q_ROWS).astype(jnp.int32) + (first >= Q_ROWS + KV_ROWS).astype(jnp.int32)


def on_device(params, deltas, momentum):
    local = deltas[0]
    _, rows, owned = momentum.shape
    half = rows // 2
    first = ((0, (), 0, rows, 1), (1, (), 0, rows, 3), (2, (0,), 0, rows, 2))
    second = ((2, (1,), 0, rows, 2),)
    flat = (rows, owned)
    b01, b03, b2, top = open_up(local, (first, second), (flat, flat, (2, *flat)))
    tops = [top, *(shift(top, d) for d in (1, 3, 2))]
    r01, r03, r2 = shift(b01, 1), shift(b03, 3), shift(b2, 2)
    b11, b13 = load((local,), ((0, 1, 1), (0, 1, 3)), (flat, flat))
    r11, r13 = shift(b11, 1), shift(b13, 3)
    y_hi = lax.axis_index("y_hi") * 2
    own_tensor = tensor_of(y_hi + lax.axis_index("y_lo"), rows)
    like = tensor_of(y_hi + lax.iota(jnp.int32, 2), rows) == own_tensor
    like = like.astype(jnp.int32)
    top = meet(tops, 32)
    tops = lax.all_to_all(top, ("y_lo", "z", "core"), 0, 0, tiled=True)
    moves = ((0, 0, 0), (1, 0, 0), (2, 0, None))
    staged0 = load((local, params, momentum), moves, [flat] * 3)
    fresh0, new0 = update(0, like, tops, (staged0[0], r01, r2, r03), *staged0[1:])
    right0, left0 = shift(fresh0, 1), shift(fresh0, 3)
    moves = ((0, 1, 0), (1, 1, 0), (2, 1, None))
    staged1 = load((local, params, momentum), moves, [flat] * 3)
    fresh1, new1 = update(1, like, tops, (staged1[0], r11, r2, r13), *staged1[1:])
    right1, left1 = shift(fresh1, 1), shift(fresh1, 3)
    farr0, farl0 = shift(right0[:half], 1), shift(left0[half:], 3)
    farr1, farl1 = shift(right1[:half], 1), shift(left1[half:], 3)
    shapes = [
        jax.ShapeDtypeStruct(params.shape, params.dtype),
        jax.ShapeDtypeStruct(momentum.shape, momentum.dtype),
    ]
    moves = [(0, l, b, 0, rows) for l in range(2) for b in (0, 3, 1)]
    moves += [(0, 0, 2, 0, half), (0, 0, 2, half, half)]
    moves += [(1, 0, 0, 0, rows), (1, 1, 0, 0, rows)]
    pieces = (fresh0, right0, left0, fresh1, right1, left1, farr0, farl0, new0, new1)
    out, new_m = place(moves, pieces, shapes, None)
    moves = [(0, 1, 2, 0, half), (0, 1, 2, half, half)]
    (out,) = place(moves, (farr1, farl1), shapes[:1], (out,))
    return out, new_m


def solution(mesh):
    torus = Mesh(mesh.devices.reshape(SIZES), AXES)
    placed = (P(None, FSDP, None), P("rep", None, FSDP, None), P(None, FSDP, "rep"))
    return jax.shard_map(
        on_device,
        mesh=torus,
        in_specs=placed,
        out_specs=(P(None, FSDP, None), P(None, FSDP, "rep")),
        check_vma=False,
    )
```

```python
import functools

import jax
import jax.numpy as jnp
from jax import lax
from jax.experimental import pallas as pl
from jax.experimental.pallas import tpu as pltpu
from jax.sharding import Mesh
from jax.sharding import PartitionSpec as P


Q_ROWS = 4096
KV_ROWS = 2048
FSDP = ("y_hi", "y_lo", "z", "core")
AXES = ("rep", *FSDP)
SIZES = (4, 2, 2, 8, 2)
REP = 4
PIECES = 4

clip_share = 0.5
peak_eps = 1e-06
outer_rate = 0.7
momentum_decay = 0.9

VMEM = pltpu.VMEM
SMALL = pltpu.CompilerParams(vmem_limit_bytes=4 * 1024 * 1024)
WHOLE = pl.BlockSpec(memory_space=pltpu.VMEM)
SCALARS = pl.BlockSpec(memory_space=pltpu.SMEM)
HBM = pl.BlockSpec(memory_space=pl.ANY)


def far(array):
    return pltpu.with_memory_space_constraint(array, pltpu.HBM)


def near(*arrays):
    return tuple(pltpu.with_memory_space_constraint(a, pltpu.VMEM) for a in arrays)


def columns(ahead, owned):
    return pl.ds(pl.multiple_of(lax.rem(lax.axis_index("rep") + ahead, REP) * owned, 128), owned)


def run_all(copies):
    for copy in copies:
        copy.start()
    for copy in copies:
        copy.wait()


def open_kernel(moves, local_ref, *refs):
    outs, (top_ref, held_ref, sems) = refs[:-3], refs[-3:]
    layers, rows, width = local_ref.shape
    owned = width // REP
    count = sems.shape[0] // layers
    step = rows // count
    loads = []
    for layer in range(layers):
        for k in range(count):
            here = (layer, pl.ds(k * step, step))
            sem = sems.at[layer * count + k]
            loads.append(pltpu.make_async_copy(local_ref.at[here], held_ref.at[here], sem))
    for load in loads:
        load.start()
    tops = []
    for layer in range(layers):
        size = None
        for k in range(count):
            loads[layer * count + k].wait()
            here = slice(k * step, (k + 1) * step)
            for which, at, first, last, ahead in moves[layer]:
                if first <= k * step < last:
                    block = held_ref[layer, here, columns(ahead, owned)]
                    outs[which][(*at, here)] = block
            chunk = jnp.max(jnp.abs(held_ref[layer, here]).reshape(step // 16, 16, width), axis=0)
            size = chunk if size is None else jnp.maximum(size, chunk)
        tops.append(jnp.max(size.astype(jnp.float32), axis=(0, 1), keepdims=True))
    lane = lax.broadcasted_iota(jnp.int32, top_ref.shape, 1)
    top_ref[...] = jnp.where(lane < top_ref.shape[1] // 2, tops[0], tops[1])


def open_up(local, moves, shapes):
    outs = [VMEM(shape, local.dtype) for shape in shapes]
    outs += [VMEM((1, 128), jnp.float32)]
    return pl.pallas_call(
        functools.partial(open_kernel, moves),
        in_specs=[HBM],
        out_specs=[WHOLE] * len(outs),
        out_shape=outs,
        scratch_shapes=[VMEM(local.shape, local.dtype), pltpu.SemaphoreType.DMA((8,))],
        compiler_params=pltpu.CompilerParams(vmem_limit_bytes=8 * 1024 * 1024),
        name="open",
    )(far(local))


def load_kernel(moves, *refs):
    count = len(moves)
    sources, outs, sems = refs[: -count - 1], refs[-count - 1 : -1], refs[-1]
    owned = outs[0].shape[-1]
    copies = []
    for k, (which, at, ahead) in enumerate(moves):
        src = sources[which].at[at]
        if ahead is not None:
            src = sources[which].at[at, :, columns(ahead, owned)]
        copies.append(pltpu.make_async_copy(src, outs[k], sems.at[k]))
    run_all(copies)


def load(sources, moves, shapes):
    return pl.pallas_call(
        functools.partial(load_kernel, moves),
        in_specs=[HBM] * len(sources),
        out_specs=[WHOLE] * len(moves),
        out_shape=[VMEM(s, sources[m[0]].dtype) for s, m in zip(shapes, moves, strict=True)],
        scratch_shapes=[pltpu.SemaphoreType.DMA((len(moves),))],
        compiler_params=SMALL,
        name="load",
    )(*map(far, sources))


def meet_kernel(*refs):
    top = functools.reduce(jnp.maximum, [ref[...] for ref in refs[:-1]])
    refs[-1][...] = jnp.broadcast_to(top[None], refs[-1].shape)


def meet(tops, count):
    return pl.pallas_call(
        meet_kernel,
        in_specs=[WHOLE] * len(tops),
        out_specs=WHOLE,
        out_shape=VMEM((count, 1, 128), jnp.float32),
        compiler_params=SMALL,
        name="meet",
    )(*near(*tops))


def tau_of(like_ref, top_ref, layer):
    mates = top_ref.shape[0] // like_ref.shape[0]
    seen = None
    for y in range(like_ref.shape[0]):
        top = jnp.max(top_ref[pl.ds(y * mates, mates)], axis=0)
        top = jnp.where(like_ref[y] == 1, top, 0.0)
        seen = top if seen is None else jnp.maximum(seen, top)
    lane = lax.broadcasted_iota(jnp.int32, seen.shape, 1)
    seen = jnp.where(lane // (seen.shape[1] // 2) == layer, seen, 0.0)
    return clip_share * (jnp.max(seen, axis=(0, 1), keepdims=True) + peak_eps)


def code_of(block, inverse):
    code = jnp.clip(block.astype(jnp.float32) * inverse, -1.0, 1.0)
    return code.astype(jnp.bfloat16).astype(jnp.float32)


def update_kernel(layer, like_ref, top_ref, *refs):
    blocks, (piece_ref, moment_ref, fresh_ref, new_ref) = refs[:-4], refs[-4:]
    tau = tau_of(like_ref, top_ref, layer)
    inverse = 1.0 / tau
    quarter = tau * (1.0 / REP)
    _, owned = fresh_ref.shape
    for start in range(0, owned, 128):
        cols = pl.ds(start, 128)
        raw = [ref[layer, :, cols] if len(ref.shape) == 3 else ref[:, cols] for ref in blocks]
        total = functools.reduce(jnp.add, [code_of(block, inverse) for block in raw])
        outer = quarter * total
        fresh_moment = momentum_decay * moment_ref[:, cols] + outer
        fresh = piece_ref[:, cols].astype(jnp.float32)
        fresh = fresh - outer_rate * (outer + momentum_decay * fresh_moment)
        fresh_ref[:, cols] = fresh.astype(jnp.bfloat16)
        new_ref[:, cols] = fresh_moment


def update(layer, like, tops, blocks, piece, moment):
    rows, owned = moment.shape
    operands = near(tops, *blocks, piece, moment)
    return pl.pallas_call(
        functools.partial(update_kernel, layer),
        in_specs=[SCALARS] + [WHOLE] * len(operands),
        out_specs=[WHOLE, WHOLE],
        out_shape=[VMEM((rows, owned), jnp.bfloat16), VMEM((rows, owned), jnp.float32)],
        compiler_params=SMALL,
    )(like, *operands)


def place_kernel(moves, count, *refs):
    sems, outs = refs[-1], refs[-1 - count : -1]
    copies = []
    for k, (which, layer, back, first, height) in enumerate(moves):
        src = refs[k]
        owned = src.shape[-1]
        here = columns(back, owned) if which == 0 else pl.ds(0, owned)
        step = height // PIECES
        for part in range(PIECES):
            dst = outs[which].at[layer, pl.ds(first + part * step, step), here]
            rows = src.at[pl.ds(part * step, step)]
            copies.append(pltpu.make_async_copy(rows, dst, sems.at[k * PIECES + part]))
    run_all(copies)


def place(moves, pieces, shapes, earlier):
    operands = list(near(*pieces))
    aliases = {}
    if earlier is not None:
        aliases = {len(operands) + k: k for k in range(len(earlier))}
        operands += earlier
    return pl.pallas_call(
        functools.partial(place_kernel, moves, len(shapes)),
        in_specs=[WHOLE] * len(pieces) + [HBM] * len(aliases),
        out_specs=[HBM] * len(shapes),
        out_shape=shapes,
        scratch_shapes=[pltpu.SemaphoreType.DMA((len(moves) * PIECES,))],
        input_output_aliases=aliases,
        compiler_params=SMALL,
        name="place",
    )(*operands)


def shift(value, by):
    return lax.ppermute(value, "rep", [(i, (i + by) % REP) for i in range(REP)])


def tensor_of(y, rows):
    first = y * SIZES[3] * SIZES[4] * rows
    return (first >= Q_ROWS).astype(jnp.int32) + (first >= Q_ROWS + KV_ROWS).astype(jnp.int32)


def on_device(params, deltas, momentum):
    local = deltas[0]
    _, rows, owned = momentum.shape
    half = rows // 2
    first = ((0, (), 0, rows, 1), (1, (), 0, rows, 3), (2, (0,), 0, rows, 2))
    second = ((2, (1,), 0, rows, 2),)
    flat = (rows, owned)
    b01, b03, b2, top = open_up(local, (first, second), (flat, flat, (2, *flat)))
    tops = [top, *(shift(top, d) for d in (1, 3, 2))]
    r01, r03, r2 = shift(b01, 1), shift(b03, 3), shift(b2, 2)
    b11, b13 = load((local,), ((0, 1, 1), (0, 1, 3)), (flat, flat))
    r11, r13 = shift(b11, 1), shift(b13, 3)
    y_hi = lax.axis_index("y_hi") * 2
    own_tensor = tensor_of(y_hi + lax.axis_index("y_lo"), rows)
    like = tensor_of(y_hi + lax.iota(jnp.int32, 2), rows) == own_tensor
    like = like.astype(jnp.int32)
    top = meet(tops, 32)
    tops = lax.all_to_all(top, ("y_lo", "z", "core"), 0, 0, tiled=True)
    moves = ((0, 0, 0), (1, 0, 0), (2, 0, None))
    staged0 = load((local, params, momentum), moves, [flat] * 3)
    fresh0, new0 = update(0, like, tops, (staged0[0], r01, r2, r03), *staged0[1:])
    right0, left0 = shift(fresh0, 1), shift(fresh0, 3)
    moves = ((0, 1, 0), (1, 1, 0), (2, 1, None))
    staged1 = load((local, params, momentum), moves, [flat] * 3)
    fresh1, new1 = update(1, like, tops, (staged1[0], r11, r2, r13), *staged1[1:])
    right1, left1 = shift(fresh1, 1), shift(fresh1, 3)
    farr0, farl0 = shift(right0[:half], 1), shift(left0[half:], 3)
    farr1, farl1 = shift(right1[:half], 1), shift(left1[half:], 3)
    shapes = [
        jax.ShapeDtypeStruct(params.shape, params.dtype),
        jax.ShapeDtypeStruct(momentum.shape, momentum.dtype),
    ]
    moves = [(0, l, b, 0, rows) for l in range(2) for b in (0, 3, 1)]
    moves += [(0, 0, 2, 0, half), (0, 0, 2, half, half)]
    moves += [(1, 0, 0, 0, rows), (1, 1, 0, 0, rows)]
    pieces = (fresh0, right0, left0, fresh1, right1, left1, farr0, farl0, new0, new1)
    out, new_m = place(moves, pieces, shapes, None)
    moves = [(0, 1, 2, 0, half), (0, 1, 2, half, half)]
    (out,) = place(moves, (farr1, farl1), shapes[:1], (out,))
    return out, new_m


def solution(mesh):
    torus = Mesh(mesh.devices.reshape(SIZES), AXES)
    placed = (P(None, FSDP, None), P("rep", None, FSDP, None), P(None, FSDP, "rep"))
    return jax.shard_map(
        on_device,
        mesh=torus,
        in_specs=placed,
        out_specs=(P(None, FSDP, None), P(None, FSDP, "rep")),
        check_vma=False,
    )
```
